16 devices in a mesh: tp: 2 (over z), fsdp: 8 (over y, x, core).
Axes of the slice: x: 2, y: 2, z: 2, core: 2. Of those that a mesh axis runs over, the one named last changes fastest.
Arguments:
- x_in: bfloat16 [128, 256, 2048], P('fsdp')
- grad_y: bfloat16 [128, 256, 2048], P('fsdp')
- w_query: bfloat16 [2048, 2048], P('fsdp', 'tp')
- w_key: bfloat16 [2048, 2048], P('fsdp', 'tp')
- w_value: bfloat16 [2048, 2048], P('fsdp', 'tp')
- w_out: bfloat16 [2048, 2048], P('tp', 'fsdp')
- w_up: bfloat16 [2048, 8192], P('fsdp', 'tp')
- b_up: float32 [8192], P('tp')
- w_down: bfloat16 [8192, 2048], P('tp', 'fsdp')
- ln_scale: float32 [2048], replicated
- q_scale: float32 [256], replicated
- k_scale: float32 [256], replicated
Outputs:
- output 1: bfloat16 [128, 256, 2048], P('fsdp')
- output 2: float32 [2048, 2048], P('fsdp', 'tp')
- output 3: float32 [2048, 2048], P('fsdp', 'tp')
- output 4: float32 [2048, 2048], P('fsdp', 'tp')
- output 5: float32 [2048, 2048], P('tp', 'fsdp')
- output 6: float32 [2048, 8192], P('fsdp', 'tp')
- output 7: float32 [8192], P('tp')
- output 8: float32 [8192, 2048], P('tp', 'fsdp')
- output 9: float32 [2048], replicated
- output 10: float32 [2048], replicated
- output 11: float32 [256], replicated
- output 12: float32 [256], replicated
All inputs are finite; a program needn't handle non-finite values.
Results may differ from the reference program's by a relative error of at most 0.02.
Values are sent between devices in bfloat16 or wider.
A program may use at most 1 GiB of HBM per device.

```python
import jax
import jax.numpy as jnp
from jax import lax

D = 2048
HEADS = 8
HEAD = 256
FF = 8192
TOKENS = 256
BATCH = 128
QKV = HEADS * HEAD
EPS = 1e-6


def scaled_norm(values, scale_vec):
    row_mean = jnp.mean(values, axis=-1, keepdims=True)
    centred = values - row_mean
    row_var = jnp.mean(centred * centred, axis=-1, keepdims=True)
    return centred * lax.rsqrt(row_var + EPS) * scale_vec


def store_bf16(values):
    return values.astype(jnp.bfloat16).astype(jnp.float32)


@jax.custom_vjp
def grad_bf16(values):
    return values


def grad_bf16_fwd(values):
    return values, None


def grad_bf16_bwd(unused, cotangent):
    return (cotangent.astype(jnp.bfloat16).astype(jnp.float32),)


grad_bf16.defvjp(grad_bf16_fwd, grad_bf16_bwd)


def setup_inputs(seed: int = 0) -> dict:
    key_list = jax.random.split(jax.random.key(seed), 12)

    def draw_normal(key_slot, shape, spread):
        return jax.random.normal(key_list[key_slot], shape, jnp.float32) * spread

    return dict(
        x_in=draw_normal(0, (BATCH, TOKENS, D), 1.0).astype(jnp.bfloat16),
        grad_y=draw_normal(1, (BATCH, TOKENS, D), 1.0).astype(jnp.bfloat16),
        w_query=draw_normal(2, (D, QKV), D ** -0.5).astype(jnp.bfloat16),
        w_key=draw_normal(3, (D, QKV), D ** -0.5).astype(jnp.bfloat16),
        w_value=draw_normal(4, (D, QKV), D ** -0.5).astype(jnp.bfloat16),
        w_out=draw_normal(5, (QKV, D), QKV ** -0.5).astype(jnp.bfloat16),
        w_up=draw_normal(6, (D, FF), D ** -0.5).astype(jnp.bfloat16),
        b_up=draw_normal(7, (FF,), 0.5),
        w_down=draw_normal(8, (FF, D), FF ** -0.5).astype(jnp.bfloat16),
        ln_scale=1.0 + draw_normal(9, (D,), 0.25),
        q_scale=1.2 + draw_normal(10, (HEAD,), 0.2),
        k_scale=1.2 + draw_normal(11, (HEAD,), 0.2),
    )


def layer_image(x_img, weights):
    w_query, w_key, w_value, w_out, w_up, b_up, w_down, ln_scale, q_scale, k_scale = weights
    x_f = x_img.astype(jnp.float32)
    normed = store_bf16(scaled_norm(x_f, ln_scale))
    q_proj = store_bf16(jnp.dot(normed, w_query)).reshape(TOKENS, HEADS, HEAD)
    k_proj = store_bf16(jnp.dot(normed, w_key)).reshape(TOKENS, HEADS, HEAD)
    v_proj = store_bf16(jnp.dot(normed, w_value)).reshape(TOKENS, HEADS, HEAD)
    q_norm = store_bf16(scaled_norm(q_proj, q_scale))
    k_norm = store_bf16(scaled_norm(k_proj, k_scale))
    logits = grad_bf16(jnp.einsum('qhd,khd->hqk', q_norm, k_norm))
    attn_prob = store_bf16(jax.nn.softmax(logits * HEAD ** -0.5, axis=-1))
    attn_out = store_bf16(jnp.einsum('hqk,khd->qhd', attn_prob, v_proj)).reshape(TOKENS, QKV)
    hidden = store_bf16(jnp.dot(normed, w_up) + b_up)
    act_out = store_bf16(jax.nn.gelu(hidden, approximate=False))
    y_out = x_f + jnp.dot(attn_out, w_out) + jnp.dot(act_out, w_down)
    return y_out.astype(jnp.bfloat16)


def reference(x_in, grad_y, w_query, w_key, w_value, w_out, w_up, b_up, w_down, ln_scale, q_scale, k_scale):
    weights = (w_query.astype(jnp.float32), w_key.astype(jnp.float32), w_value.astype(jnp.float32),
               w_out.astype(jnp.float32), w_up.astype(jnp.float32), b_up, w_down.astype(jnp.float32),
               ln_scale, q_scale, k_scale)

    def run_all(x_all, weight_set):
        def one_image(x_img):
            return layer_image(x_img, weight_set)
        return lax.map(jax.checkpoint(one_image), x_all)

    y_unused, pullback = jax.vjp(run_all, x_in, weights)
    grad_x, grad_w = pullback(grad_y)
    grad_b_down = jnp.sum(grad_y.astype(jnp.float32), axis=(0, 1))
    return (grad_x, grad_w[0], grad_w[1], grad_w[2], grad_w[3], grad_w[4], grad_w[5], grad_w[6],
            grad_b_down, grad_w[7], grad_w[8], grad_w[9])
```

```python
import functools
import jax
import jax.numpy as jnp
from jax import lax
from jax.experimental import pallas as pl
from jax.experimental.pallas import tpu as pltpu
from jax.sharding import PartitionSpec as P

EPS = 1e-6
bf16 = jnp.bfloat16
fp32 = jnp.float32
CHUNKS = 4


def dot_nn(a, b):
    return lax.dot_general(a, b, (((1,), (0,)), ((), ())), preferred_element_type=fp32)


def dot_nt(a, b):
    return lax.dot_general(a, b, (((1,), (1,)), ((), ())), preferred_element_type=fp32)


def dot_tn(a, b):
    return lax.dot_general(a, b, (((0,), (0,)), ((), ())), preferred_element_type=fp32)


def norm_parts(values):
    centred = values - jnp.mean(values, axis=-1, keepdims=True)
    inv = lax.rsqrt(jnp.mean(centred * centred, axis=-1, keepdims=True) + EPS)
    return centred * inv, inv


def norm_back(unit, inv, gain, cot):
    d_unit = cot * gain
    m_one = jnp.mean(d_unit, axis=-1, keepdims=True)
    m_two = jnp.mean(d_unit * unit, axis=-1, keepdims=True)
    return inv * (d_unit - m_one - unit * m_two)


def attn_kernel(heads, dim, q_ref, k_ref, v_ref, do_ref, gq_ref, gk_ref, o_ref, dqkv_ref, dgq_ref, dgk_ref):
    @pl.when(pl.program_id(0) == 0)
    def _():
        dgq_ref[...] = jnp.zeros_like(dgq_ref)
        dgk_ref[...] = jnp.zeros_like(dgk_ref)

    scale = dim ** -0.5
    width = heads * dim
    gain_q = gq_ref[...]
    gain_k = gk_ref[...]
    tot_q = jnp.zeros((8, dim), fp32)
    tot_k = jnp.zeros((8, dim), fp32)
    for head in range(heads):
        cols = slice(head * dim, (head + 1) * dim)
        q_unit, q_inv = norm_parts(q_ref[:, cols].astype(fp32))
        k_unit, k_inv = norm_parts(k_ref[:, cols].astype(fp32))
        q_norm = (q_unit * gain_q).astype(bf16)
        k_norm = (k_unit * gain_k).astype(bf16)
        val = v_ref[:, cols]
        d_out = do_ref[:, cols]
        logit_t = dot_nt(k_norm, q_norm) * scale
        expo = jnp.exp(logit_t - jnp.max(logit_t, axis=0, keepdims=True))
        prob_t = expo / jnp.sum(expo, axis=0, keepdims=True)
        prob_b = prob_t.astype(bf16)
        o_ref[:, cols] = dot_tn(prob_b, val).astype(bf16)
        d_prob = dot_nt(val, d_out).astype(bf16).astype(fp32)
        dqkv_ref[:, 2 * width + head * dim:2 * width + (head + 1) * dim] = dot_nn(prob_b, d_out).astype(bf16)
        row = jnp.sum(prob_t * d_prob, axis=0, keepdims=True)
        d_logit = (prob_t * (d_prob - row) * scale).astype(bf16)
        d_qn = dot_tn(d_logit, k_norm).astype(bf16).astype(fp32)
        d_kn = dot_nn(d_logit, q_norm).astype(bf16).astype(fp32)
        dqkv_ref[:, cols] = norm_back(q_unit, q_inv, gain_q, d_qn).astype(bf16)
        dqkv_ref[:, width + head * dim:width + (head + 1) * dim] = norm_back(k_unit, k_inv, gain_k, d_kn).astype(bf16)
        tot_q = tot_q + jnp.sum((d_qn * q_unit).reshape(-1, 8, dim), axis=0)
        tot_k = tot_k + jnp.sum((d_kn * k_unit).reshape(-1, 8, dim), axis=0)
    dgq_ref[...] += tot_q
    dgk_ref[...] += tot_k


def attention(qkv, d_attn, q_scale, k_scale, num_img):
    total, width3 = qkv.shape
    width = width3 // 3
    dim = q_scale.shape[0]
    tok = total // num_img
    heads = width // dim
    part = lambda col: pl.BlockSpec((tok, width), lambda i, col=col: (i, col))
    whole = lambda rows: pl.BlockSpec((rows, dim), lambda i: (0, 0))
    return pl.pallas_call(
        functools.partial(attn_kernel, heads, dim),
        grid=(num_img,),
        in_specs=[part(0), part(1), part(2), part(0), whole(1), whole(1)],
        out_specs=[part(0), pl.BlockSpec((tok, width3), lambda i: (i, 0)), whole(8), whole(8)],
        out_shape=[jax.ShapeDtypeStruct((total, width), bf16), jax.ShapeDtypeStruct((total, width3), bf16),
                   jax.ShapeDtypeStruct((8, dim), fp32), jax.ShapeDtypeStruct((8, dim), fp32)],
        compiler_params=pltpu.CompilerParams(dimension_semantics=("arbitrary",), vmem_limit_bytes=56 * 2 ** 20),
        cost_estimate=pl.CostEstimate(flops=5 * 12 * total * tok * width, bytes_accessed=16 * total * width,
                                      transcendentals=total * tok * heads),
        name="attn",
    )(qkv, qkv, qkv, d_attn, q_scale.reshape(1, dim), k_scale.reshape(1, dim))


def mlp_kernel(sub, h_ref, gy_ref, wu_ref, wd_ref, b_ref, act_ref, dh_ref, db_ref):
    @pl.when(pl.program_id(1) == 0)
    def _():
        db_ref[...] = jnp.zeros_like(db_ref)

    h = h_ref[...]
    gy = gy_ref[...]
    for start in range(0, act_ref.shape[1], sub):
        cols = slice(start, start + sub)
        hid = (dot_nn(h, wu_ref[:, cols]) + b_ref[:, cols]).astype(bf16).astype(fp32)
        d_act = dot_nt(gy, wd_ref[cols, :]).astype(bf16).astype(fp32)
        cdf = 0.5 + 0.5 * lax.erf(hid * (0.5 ** 0.5))
        pdf = jnp.exp(hid * hid * -0.5) * 0.3989422804014327
        act_ref[:, cols] = (hid * cdf).astype(bf16)
        d_hid = (d_act * (cdf + hid * pdf)).astype(bf16)
        dh_ref[:, cols] = d_hid
        db_ref[:, cols] += jnp.sum(d_hid.astype(fp32).reshape(-1, 8, sub), axis=0)


def mlp(normed, grad_y, w_up, w_down, b_up, rows, cols, sub):
    total, depth = normed.shape
    width = w_up.shape[1]
    row_spec = pl.BlockSpec((rows, depth), lambda j, i: (i, 0))
    out_spec = pl.BlockSpec((rows, cols), lambda j, i: (i, j))
    return pl.pallas_call(
        functools.partial(mlp_kernel, sub),
        grid=(width // cols, total // rows),
        in_specs=[row_spec, row_spec, pl.BlockSpec((depth, cols), lambda j, i: (0, j)),
                  pl.BlockSpec((cols, depth), lambda j, i: (j, 0)), pl.BlockSpec((1, cols), lambda j, i: (0, j))],
        out_specs=[out_spec, out_spec, pl.BlockSpec((8, cols), lambda j, i: (0, j))],
        out_shape=[jax.ShapeDtypeStruct((total, width), bf16), jax.ShapeDtypeStruct((total, width), bf16),
                   jax.ShapeDtypeStruct((8, width), fp32)],
        compiler_params=pltpu.CompilerParams(dimension_semantics=("arbitrary", "arbitrary"),
                                             vmem_limit_bytes=60 * 2 ** 20),
        cost_estimate=pl.CostEstimate(flops=4 * total * depth * width, bytes_accessed=16 * total * width,
                                      transcendentals=2 * total * width),
        name="mlp",
    )(normed, grad_y, w_up, w_down, b_up.reshape(1, width))


def after(value, *earlier):
    return lax.optimization_barrier((value,) + earlier)[0]


def solution(mesh):
    act_spec = P('fsdp', None, None)
    row_spec = P('fsdp', 'tp')
    col_spec = P('tp', 'fsdp')
    in_specs = (act_spec, act_spec, row_spec, row_spec, row_spec, col_spec, row_spec, P('tp'), col_spec, P(), P(), P())
    out_specs = (act_spec, row_spec, row_spec, row_spec, col_spec, row_spec, P('tp'), col_spec, P(), P(), P(), P())
    gather_rows = functools.partial(lax.all_gather, axis_name='fsdp', axis=0, tiled=True)
    gather_cols = functools.partial(lax.all_gather, axis_name='fsdp', axis=1, tiled=True)
    scatter_rows = functools.partial(lax.psum_scatter, axis_name='fsdp', scatter_dimension=0, tiled=True)
    scatter_cols = functools.partial(lax.psum_scatter, axis_name='fsdp', scatter_dimension=1, tiled=True)
    num_tp = mesh.shape['tp']
    swap = [(i, num_tp - 1 - i) for i in range(num_tp)]

    def local_step(x_in, grad_y, w_query, w_key, w_value, w_out, w_up, b_up, w_down, ln_scale, q_scale, k_scale):
        num_img, num_tok, depth = x_in.shape
        total = num_img * num_tok
        width = w_query.shape[1]
        x2 = x_in.reshape(total, depth)
        gy2 = grad_y.reshape(total, depth)
        tp_idx = lax.axis_index('tp')

        w_qkv = gather_rows(jnp.concatenate([w_query, w_key, w_value], axis=1))
        wo = gather_cols(w_out)
        wu = gather_rows(w_up)
        wd = gather_cols(w_down)

        unit, _ = norm_parts(x2.astype(fp32))
        normed = (unit * ln_scale).astype(bf16)
        b_down_part = jnp.sum(gy2, axis=0, dtype=fp32)
        normed, b_down_part = lax.optimization_barrier((normed, b_down_part))

        qkv = dot_nn(normed, w_qkv).astype(bf16)
        d_attn = dot_nt(after(gy2, qkv), wo).astype(bf16)
        attn_out, d_qkv, dgq, dgk = attention(qkv, d_attn, q_scale, k_scale, num_img)
        gw_out = dot_tn(attn_out, gy2)
        gw_qkv = dot_tn(normed, after(d_qkv, gw_out))

        act_out, d_hid, db_part = mlp(after(normed, gw_qkv), gy2, wu, wd, b_up, 512, 1024, 256)

        rows = total // CHUNKS
        half = rows // num_tp
        mine = tp_idx * half
        theirs = (num_tp - 1) * half - mine

        def d_normed_of(chunk, hid):
            part = slice(chunk * rows, (chunk + 1) * rows)
            return dot_nt(hid[part], wu) + dot_nt(d_qkv[part], w_qkv)

        def exchange(d_norm):
            return lax.ppermute(lax.dynamic_slice_in_dim(d_norm, theirs, half), 'tp', swap)

        def finish(chunk, d_norm, other):
            own = lax.dynamic_slice_in_dim(d_norm, mine, half)
            cot = (own + other).astype(bf16).astype(fp32)
            begin = chunk * rows + mine
            x_unit, x_inv = norm_parts(lax.dynamic_slice_in_dim(x2, begin, half).astype(fp32))
            d_x = norm_back(x_unit, x_inv, ln_scale, cot)
            g_x = (lax.dynamic_slice_in_dim(gy2, begin, half).astype(fp32) + d_x).astype(bf16)
            return g_x, jnp.sum(cot * x_unit, axis=0)

        dn0 = d_normed_of(0, d_hid)
        got0 = exchange(dn0)
        dn1 = d_normed_of(1, after(d_hid, dn0))
        got1 = exchange(dn1)
        gw_down = dot_tn(after(act_out, dn1), gy2)
        dn2 = d_normed_of(2, after(d_hid, gw_down))
        got2 = exchange(dn2)
        dn3 = d_normed_of(3, after(d_hid, dn2))
        got3 = exchange(dn3)
        gx0, ls0 = finish(0, dn0, after(got0, dn3))
        gx1, ls1 = finish(1, dn1, after(got1, dn3))
        gw_up = dot_tn(normed, after(d_hid, dn3, gx0, gx1))
        gx2, ls2 = finish(2, dn2, after(got2, gw_up))
        gx3, ls3 = finish(3, dn3, after(got3, gw_up))

        own_parts = (gx0, gx1, gx2, gx3)
        back_parts = []
        for piece in own_parts:
            back_parts.append(lax.ppermute(piece, 'tp', swap))
        own_parts, back_parts = lax.optimization_barrier((own_parts, tuple(back_parts)))
        pieces = []
        for own, back in zip(own_parts, back_parts):
            pieces += [jnp.where(tp_idx == 0, own, back), jnp.where(tp_idx == 0, back, own)]
        grad_x = jnp.concatenate(pieces, axis=0)

        first = (tp_idx == 0).astype(fp32)
        b_up_slots = jnp.zeros((num_tp, b_up.shape[0]), fp32)
        b_up_slots = lax.dynamic_update_slice_in_dim(b_up_slots, jnp.sum(db_part, axis=0, keepdims=True), tp_idx, 0)
        small = lax.psum(jnp.concatenate([b_up_slots.reshape(-1), b_down_part * first, ls0 + ls1 + ls2 + ls3,
                                          jnp.sum(dgq, axis=0), jnp.sum(dgk, axis=0)]), ('tp', 'fsdp'))
        ends = [num_tp * b_up.shape[0], depth, depth, q_scale.shape[0], k_scale.shape[0]]
        spans, at = [], 0
        for size in ends:
            spans.append(small[at:at + size])
            at += size
        g_b_up = lax.dynamic_slice_in_dim(spans[0], tp_idx * b_up.shape[0], b_up.shape[0])

        s_out = scatter_cols(gw_out)
        s_qkv = scatter_rows(gw_qkv)
        s_down = scatter_cols(gw_down)
        s_up = scatter_rows(gw_up)
        return (grad_x.reshape(x_in.shape), s_qkv[:, :width], s_qkv[:, width:2 * width], s_qkv[:, 2 * width:],
                s_out, s_up, g_b_up, s_down, spans[1], spans[2], spans[3], spans[4])

    return jax.shard_map(local_step, mesh=mesh, in_specs=in_specs, out_specs=out_specs, check_vma=False)
```

```python
import functools
import jax
import jax.numpy as jnp
from jax import lax
from jax.experimental import pallas as pl
from jax.experimental.pallas import tpu as pltpu
from jax.sharding import PartitionSpec as P

EPS = 1e-6
bf16 = jnp.bfloat16
fp32 = jnp.float32
CHUNKS = 4


def dot_nn(a, b):
    return lax.dot_general(a, b, (((1,), (0,)), ((), ())), preferred_element_type=fp32)


def dot_nt(a, b):
    return lax.dot_general(a, b, (((1,), (1,)), ((), ())), preferred_element_type=fp32)


def dot_tn(a, b):
    return lax.dot_general(a, b, (((0,), (0,)), ((), ())), preferred_element_type=fp32)


def norm_parts(values):
    centred = values - jnp.mean(values, axis=-1, keepdims=True)
    inv = lax.rsqrt(jnp.mean(centred * centred, axis=-1, keepdims=True) + EPS)
    return centred * inv, inv


def norm_back(unit, inv, gain, cot):
    d_unit = cot * gain
    m_one = jnp.mean(d_unit, axis=-1, keepdims=True)
    m_two = jnp.mean(d_unit * unit, axis=-1, keepdims=True)
    return inv * (d_unit - m_one - unit * m_two)


def attn_kernel(heads, dim, q_ref, k_ref, v_ref, do_ref, gq_ref, gk_ref, o_ref, dqkv_ref, dgq_ref, dgk_ref):
    @pl.when(pl.program_id(0) == 0)
    def _():
        dgq_ref[...] = jnp.zeros_like(dgq_ref)
        dgk_ref[...] = jnp.zeros_like(dgk_ref)

    scale = dim ** -0.5
    width = heads * dim
    gain_q = gq_ref[...]
    gain_k = gk_ref[...]
    tot_q = jnp.zeros((8, dim), fp32)
    tot_k = jnp.zeros((8, dim), fp32)
    for head in range(heads):
        cols = slice(head * dim, (head + 1) * dim)
        q_unit, q_inv = norm_parts(q_ref[:, cols].astype(fp32))
        k_unit, k_inv = norm_parts(k_ref[:, cols].astype(fp32))
        q_norm = (q_unit * gain_q).astype(bf16)
        k_norm = (k_unit * gain_k).astype(bf16)
        val = v_ref[:, cols]
        d_out = do_ref[:, cols]
        logit_t = dot_nt(k_norm, q_norm) * scale
        expo = jnp.exp(logit_t - jnp.max(logit_t, axis=0, keepdims=True))
        prob_t = expo / jnp.sum(expo, axis=0, keepdims=True)
        prob_b = prob_t.astype(bf16)
        o_ref[:, cols] = dot_tn(prob_b, val).astype(bf16)
        d_prob = dot_nt(val, d_out).astype(bf16).astype(fp32)
        dqkv_ref[:, 2 * width + head * dim:2 * width + (head + 1) * dim] = dot_nn(prob_b, d_out).astype(bf16)
        row = jnp.sum(prob_t * d_prob, axis=0, keepdims=True)
        d_logit = (prob_t * (d_prob - row) * scale).astype(bf16)
        d_qn = dot_tn(d_logit, k_norm).astype(bf16).astype(fp32)
        d_kn = dot_nn(d_logit, q_norm).astype(bf16).astype(fp32)
        dqkv_ref[:, cols] = norm_back(q_unit, q_inv, gain_q, d_qn).astype(bf16)
        dqkv_ref[:, width + head * dim:width + (head + 1) * dim] = norm_back(k_unit, k_inv, gain_k, d_kn).astype(bf16)
        tot_q = tot_q + jnp.sum((d_qn * q_unit).reshape(-1, 8, dim), axis=0)
        tot_k = tot_k + jnp.sum((d_kn * k_unit).reshape(-1, 8, dim), axis=0)
    dgq_ref[...] += tot_q
    dgk_ref[...] += tot_k


def attention(qkv, d_attn, q_scale, k_scale, num_img):
    total, width3 = qkv.shape
    width = width3 // 3
    dim = q_scale.shape[0]
    tok = total // num_img
    heads = width // dim
    part = lambda col: pl.BlockSpec((tok, width), lambda i, col=col: (i, col))
    whole = lambda rows: pl.BlockSpec((rows, dim), lambda i: (0, 0))
    return pl.pallas_call(
        functools.partial(attn_kernel, heads, dim),
        grid=(num_img,),
        in_specs=[part(0), part(1), part(2), part(0), whole(1), whole(1)],
        out_specs=[part(0), pl.BlockSpec((tok, width3), lambda i: (i, 0)), whole(8), whole(8)],
        out_shape=[jax.ShapeDtypeStruct((total, width), bf16), jax.ShapeDtypeStruct((total, width3), bf16),
                   jax.ShapeDtypeStruct((8, dim), fp32), jax.ShapeDtypeStruct((8, dim), fp32)],
        compiler_params=pltpu.CompilerParams(dimension_semantics=("arbitrary",), vmem_limit_bytes=56 * 2 ** 20),
        cost_estimate=pl.CostEstimate(flops=5 * 12 * total * tok * width, bytes_accessed=16 * total * width,
                                      transcendentals=total * tok * heads),
        name="attn",
    )(qkv, qkv, qkv, d_attn, q_scale.reshape(1, dim), k_scale.reshape(1, dim))


def mlp_kernel(sub, h_ref, gy_ref, wu_ref, wd_ref, b_ref, *refs):
    act_ref, dh_ref, db_ref = refs[-3:]

    @pl.when(pl.program_id(1) == 0)
    def _():
        db_ref[...] = jnp.zeros_like(db_ref)

    h = h_ref[...]
    gy = gy_ref[...]
    for start in range(0, act_ref.shape[1], sub):
        cols = slice(start, start + sub)
        hid = (dot_nn(h, wu_ref[:, cols]) + b_ref[:, cols]).astype(bf16).astype(fp32)
        d_act = dot_nt(gy, wd_ref[cols, :]).astype(bf16).astype(fp32)
        cdf = 0.5 + 0.5 * lax.erf(hid * (0.5 ** 0.5))
        pdf = jnp.exp(hid * hid * -0.5) * 0.3989422804014327
        act_ref[:, cols] = (hid * cdf).astype(bf16)
        d_hid = (d_act * (cdf + hid * pdf)).astype(bf16)
        dh_ref[:, cols] = d_hid
        db_ref[:, cols] += jnp.sum(d_hid.astype(fp32).reshape(-1, 8, sub), axis=0)


def mlp(normed, grad_y, w_up, w_down, b_up, rows, cols, sub, part, parts, held):
    total, depth = normed.shape
    width = w_up.shape[1]
    steps = total // rows // parts
    skip = part * steps
    row_spec = pl.BlockSpec((rows, depth), lambda j, i: (i + skip, 0))
    out_spec = pl.BlockSpec((rows, cols), lambda j, i: (i + skip, j))
    return pl.pallas_call(
        functools.partial(mlp_kernel, sub),
        grid=(width // cols, steps),
        in_specs=[row_spec, row_spec, pl.BlockSpec((depth, cols), lambda j, i: (0, j)),
                  pl.BlockSpec((cols, depth), lambda j, i: (j, 0)), pl.BlockSpec((1, cols), lambda j, i: (0, j))]
        + [pl.BlockSpec(memory_space=pl.ANY)] * len(held),
        out_specs=[out_spec, out_spec, pl.BlockSpec((8, cols), lambda j, i: (0, j))],
        out_shape=[jax.ShapeDtypeStruct((total, width), bf16), jax.ShapeDtypeStruct((total, width), bf16),
                   jax.ShapeDtypeStruct((8, width), fp32)],
        input_output_aliases={5 + n: n for n in range(len(held))},
        compiler_params=pltpu.CompilerParams(dimension_semantics=("arbitrary", "arbitrary"),
                                             vmem_limit_bytes=60 * 2 ** 20),
        cost_estimate=pl.CostEstimate(flops=4 * total * depth * width // parts,
                                      bytes_accessed=16 * total * width // parts,
                                      transcendentals=2 * total * width // parts),
        name="mlp",
    )(normed, grad_y, w_up, w_down, b_up.reshape(1, width), *held)


def after(value, *earlier):
    return lax.optimization_barrier((value,) + earlier)[0]


def solution(mesh):
    act_spec = P('fsdp', None, None)
    row_spec = P('fsdp', 'tp')
    col_spec = P('tp', 'fsdp')
    in_specs = (act_spec, act_spec, row_spec, row_spec, row_spec, col_spec, row_spec, P('tp'), col_spec, P(), P(), P())
    out_specs = (act_spec, row_spec, row_spec, row_spec, col_spec, row_spec, P('tp'), col_spec, P(), P(), P(), P())
    gather_rows = functools.partial(lax.all_gather, axis_name='fsdp', axis=0, tiled=True)
    gather_cols = functools.partial(lax.all_gather, axis_name='fsdp', axis=1, tiled=True)
    scatter_rows = functools.partial(lax.psum_scatter, axis_name='fsdp', scatter_dimension=0, tiled=True)
    scatter_cols = functools.partial(lax.psum_scatter, axis_name='fsdp', scatter_dimension=1, tiled=True)
    num_tp = mesh.shape['tp']
    num_fsdp = mesh.shape['fsdp']
    swap = [(i, num_tp - 1 - i) for i in range(num_tp)]

    def local_step(x_in, grad_y, w_query, w_key, w_value, w_out, w_up, b_up, w_down, ln_scale, q_scale, k_scale):
        num_img, num_tok, depth = x_in.shape
        total = num_img * num_tok
        width = w_query.shape[1]
        x2 = x_in.reshape(total, depth)
        gy2 = grad_y.reshape(total, depth)
        tp_idx = lax.axis_index('tp')

        w_qkv = gather_rows(jnp.concatenate([w_query, w_key, w_value], axis=1))
        wo = gather_cols(w_out)
        wu = gather_rows(w_up)
        wd = gather_cols(w_down)

        unit, _ = norm_parts(x2.astype(fp32))
        normed = (unit * ln_scale).astype(bf16)
        b_down_part = jnp.sum(gy2, axis=0, dtype=fp32)
        normed, b_down_part = lax.optimization_barrier((normed, b_down_part))

        qkv = dot_nn(normed, w_qkv).astype(bf16)
        d_attn = dot_nt(after(gy2, qkv), wo).astype(bf16)
        attn_out, d_qkv, dgq, dgk = attention(qkv, d_attn, q_scale, k_scale, num_img)
        gw_out = dot_tn(attn_out, gy2)
        gw_qkv = dot_tn(normed, after(d_qkv, gw_out))

        def mlp_part(part, start, held):
            return mlp(start, gy2, wu, wd, b_up, 512, 1024, 256, part, 2, held)

        rows = total // CHUNKS
        half = rows // num_tp
        mine = tp_idx * half
        theirs = (num_tp - 1) * half - mine

        def d_normed_of(chunk, hid):
            part = slice(chunk * rows, (chunk + 1) * rows)
            return dot_nt(hid[part], wu) + dot_nt(d_qkv[part], w_qkv)

        def exchange(d_norm):
            return lax.ppermute(lax.dynamic_slice_in_dim(d_norm, theirs, half), 'tp', swap)

        def finish(chunk, d_norm, other):
            own = lax.dynamic_slice_in_dim(d_norm, mine, half)
            cot = (own + other).astype(bf16).astype(fp32)
            begin = chunk * rows + mine
            x_unit, x_inv = norm_parts(lax.dynamic_slice_in_dim(x2, begin, half).astype(fp32))
            d_x = norm_back(x_unit, x_inv, ln_scale, cot)
            g_x = (lax.dynamic_slice_in_dim(gy2, begin, half).astype(fp32) + d_x).astype(bf16)
            return g_x, jnp.sum(cot * x_unit, axis=0)

        act_half, hid_half, db0 = mlp_part(0, after(normed, gw_qkv), ())
        dn0 = d_normed_of(0, hid_half)
        got0 = exchange(dn0)
        dn1 = d_normed_of(1, after(hid_half, dn0))
        got1 = exchange(dn1)
        act_out, d_hid, db1 = mlp_part(1, after(normed, dn0, dn1), (act_half, hid_half))
        gx0, ls0 = finish(0, dn0, after(got0, db1))
        gw_down = dot_tn(act_out, after(gy2, gx0))
        gx1, ls1 = finish(1, dn1, after(got1, gw_down))
        dn2 = d_normed_of(2, after(d_hid, gw_down))
        got2 = exchange(dn2)
        dn3 = d_normed_of(3, after(d_hid, dn2))
        got3 = exchange(dn3)
        gw_up = dot_tn(normed, after(d_hid, dn3, gx1))
        gx2, ls2 = finish(2, dn2, after(got2, gw_up))
        gx3, ls3 = finish(3, dn3, after(got3, gx2))

        own_parts = (gx0, gx1, gx2, gx3)
        back_parts = []
        for piece in own_parts:
            back_parts.append(lax.ppermute(piece, 'tp', swap))
        own_parts, back_parts = lax.optimization_barrier((own_parts, tuple(back_parts)))
        pieces = []
        for own, back in zip(own_parts, back_parts):
            pieces += [jnp.where(tp_idx == 0, own, back), jnp.where(tp_idx == 0, back, own)]
        grad_x = jnp.concatenate(pieces, axis=0)

        first = (tp_idx == 0).astype(fp32)
        b_up_slots = jnp.zeros((num_tp, b_up.shape[0]), fp32)
        b_up_slots = lax.dynamic_update_slice_in_dim(b_up_slots, jnp.sum(db0 + db1, axis=0, keepdims=True), tp_idx, 0)
        small = jnp.concatenate([b_up_slots.reshape(-1), b_down_part * first, ls0 + ls1 + ls2 + ls3,
                                 jnp.sum(dgq, axis=0), jnp.sum(dgk, axis=0)])
        bit = 1
        while bit < num_fsdp:
            small = small + lax.ppermute(small, 'fsdp', [(i, i ^ bit) for i in range(num_fsdp)])
            bit *= 2
        small = small + lax.ppermute(small, 'tp', swap)
        ends = [num_tp * b_up.shape[0], depth, depth, q_scale.shape[0], k_scale.shape[0]]
        spans, at = [], 0
        for size in ends:
            spans.append(small[at:at + size])
            at += size
        g_b_up = lax.dynamic_slice_in_dim(spans[0], tp_idx * b_up.shape[0], b_up.shape[0])

        s_out = scatter_cols(gw_out)
        s_qkv = scatter_rows(gw_qkv)
        s_down = scatter_cols(gw_down)
        s_up = scatter_rows(gw_up)
        return (grad_x.reshape(x_in.shape), s_qkv[:, :width], s_qkv[:, width:2 * width], s_qkv[:, 2 * width:],
                s_out, s_up, g_b_up, s_down, spans[1], spans[2], spans[3], spans[4])

    return jax.shard_map(local_step, mesh=mesh, in_specs=in_specs, out_specs=out_specs, check_vma=False)
```
